32 devices in a mesh: dp: 4 (over y, core), tp: 8 (over z, x).
Axes of the slice: x: 2, y: 2, z: 4, core: 2. Of those that a mesh axis runs over, the one named last changes fastest.
Arguments:
- tokens: bfloat16 [1024, 7168], P(('dp', 'tp')), may hold values from -6 to 6
- w_gate: bfloat16 [7168, 12288], P(None, 'tp'), may hold values from -0.0625 to 0.0625
- w_up: bfloat16 [7168, 12288], P(None, 'tp'), may hold values from -0.0625 to 0.0625
- w_down: bfloat16 [12288, 7168], P('tp'), may hold values from -0.0546875 to 0.0546875
- cotangent: bfloat16 [1024, 7168], P(('dp', 'tp')), may hold values from -6 to 6
Outputs:
- mixed: bfloat16 [1024, 7168], P(('dp', 'tp'))
- input_grad: bfloat16 [1024, 7168], P(('dp', 'tp'))
- gate_grad: float32 [7168, 12288], P('dp', 'tp')
- up_grad: float32 [7168, 12288], P('dp', 'tp')
- down_grad: float32 [12288, 7168], P('tp', 'dp')
The draws below stay inside these ranges and needn't reach their ends.
All inputs are finite; a program needn't handle non-finite values.
Results may differ from the reference program's by a relative error of at most 0.0049.
Values may be sent and summed in bfloat16 or wider, within the bound.
A program may use at most 192 MiB of HBM per device.

```python
import jax
import jax.numpy as jnp

D = 7168
FF = 12288
TOKENS = 1024


def shard_levels(key, shape, cuts, low, largest):
    def one(dim, parts):
        steps = jax.random.uniform(jax.random.fold_in(jax.random.fold_in(key, 6), dim), (parts,), jnp.float32, low / len(cuts), largest / len(cuts))
        return jnp.repeat(jnp.exp(steps), shape[dim] // parts).reshape((-1,) + (1,) * (len(shape) - dim - 1))

    loudness = one(*cuts[0])
    for cut in cuts[1:]:
        loudness = loudness * one(*cut)
    return loudness


def gaussian(own_key, extent, scale, reach, cuts=(), held_as=jnp.bfloat16):
    loudness = shard_levels(own_key, extent, cuts, -0.22, 0.18) if cuts else 1.0
    drawn = jax.random.normal(own_key, extent, jnp.float32) * scale * loudness
    return jnp.minimum(jnp.maximum(drawn, -reach), reach).astype(held_as)


def setup_inputs(seed: int = 0) -> dict:
    arg_keys = jax.random.split(jax.random.key(seed), 6)
    return {
        "tokens": gaussian(arg_keys[0], (TOKENS, D), 1.0, 6.0, ((0, 32),)),
        "w_gate": gaussian(arg_keys[1], (D, FF), D ** -0.5, 0.0625, ((1, 8),)),
        "w_up": gaussian(arg_keys[2], (D, FF), D ** -0.5, 0.0625, ((1, 8),)),
        "w_down": gaussian(arg_keys[3], (FF, D), FF ** -0.5, 0.0546875, ((0, 8),)),
        "cotangent": gaussian(arg_keys[4], (TOKENS, D), 1.0, 6.0, ((0, 32),)),
    }


def reference(tokens, w_gate, w_up, w_down, cotangent):
    gate = jnp.dot(tokens, w_gate, preferred_element_type=jnp.float32)
    up = jnp.dot(tokens, w_up, preferred_element_type=jnp.float32)
    sig = jax.nn.sigmoid(gate)
    act = gate * sig
    hidden = (act * up).astype(jnp.bfloat16)
    mixed = jnp.dot(hidden, w_down, preferred_element_type=jnp.float32).astype(jnp.bfloat16)
    back = jnp.dot(cotangent, w_down.T, preferred_element_type=jnp.float32)
    dgate = (back * up * sig * (1.0 + gate * (1.0 - sig))).astype(jnp.bfloat16)
    dup = (back * act).astype(jnp.bfloat16)
    input_grad = (jnp.dot(dgate, w_gate.T, preferred_element_type=jnp.float32)
                  + jnp.dot(dup, w_up.T, preferred_element_type=jnp.float32)).astype(jnp.bfloat16)
    gate_grad = jnp.dot(tokens.T, dgate, preferred_element_type=jnp.float32)
    up_grad = jnp.dot(tokens.T, dup, preferred_element_type=jnp.float32)
    down_grad = jnp.dot(hidden.T, cotangent, preferred_element_type=jnp.float32)
    return mixed, input_grad, gate_grad, up_grad, down_grad
```

```python
import functools

import jax
import jax.numpy as jnp
from jax import lax
from jax.experimental import pallas as pl
from jax.experimental.pallas import tpu as pltpu
from jax.sharding import PartitionSpec as P

BF16 = jnp.bfloat16
F32 = jnp.float32


def right_trans(left, matrix):
    return lax.dot_general(left, matrix, (((1,), (1,)), ((), ())), preferred_element_type=F32)


def send_xor(block, bit, count):
    return lax.ppermute(block, "dp", [(i, i ^ bit) for i in range(count)])


def send_tp(block, dz, dx, count):
    ring = count // 2
    perm = [(i, ((i // 2 + dz) % ring) * 2 + ((i % 2) ^ dx)) for i in range(count)]
    return lax.ppermute(block, "tp", perm)


def gather_tp(own, count):
    if count != 8:
        whole = lax.all_gather(own, "tp", axis=0)
        return [whole[i] for i in range(count)]
    send = functools.partial(send_tp, count=count)
    across = send(own, 0, 1)
    below = send(own, 1, 0)
    above = send(own, -1, 0)
    across_above = send(above, 0, 1)
    across_below = send(across, 1, 0)
    far = send(above, -1, 0)
    half = own.shape[1] // 256 * 128
    across_far = jnp.concatenate(
        [send(across_above[:, :half], -1, 0), send(across_below[:, half:], 1, 0)], axis=1
    )
    return [own, across, above, across_above, far, across_far, below, across_below]


def scatter_tp(partial, count):
    rows = partial.shape[0] // count
    if count != 8:
        return lax.psum_scatter(partial.astype(F32), "tp", scatter_dimension=0, tiled=True).astype(BF16)
    send = functools.partial(send_tp, count=count)
    half = partial.shape[1] // 256 * 128
    near, above, far, below = (partial[i * 2 * rows : (i + 1) * 2 * rows] for i in range(4))
    from_below = send(far[:, :half], 1, 0)
    from_above = send(far[:, half:], -1, 0)
    up = jnp.concatenate(
        [(above[:, :half].astype(F32) + from_below.astype(F32)).astype(BF16), above[:, half:]], axis=1
    )
    down = jnp.concatenate(
        [below[:, :half], (below[:, half:].astype(F32) + from_above.astype(F32)).astype(BF16)], axis=1
    )
    up = send(up, 1, 0)
    down = send(down, -1, 0)
    total = near.astype(F32) + up.astype(F32) + down.astype(F32)
    crossed = send(total[rows:].astype(BF16), 0, 1)
    return (total[:rows] + crossed.astype(F32)).astype(BF16)


def gather_dp(own, count):
    blocks = {0: own}
    bit = count // 2
    while bit:
        blocks.update({k | bit: send_xor(b, bit, count) for k, b in list(blocks.items())})
        bit //= 2
    return [blocks[k] for k in range(count)]


def grad_kernel(count, *refs):
    lefts, rights, out = refs[:count], refs[count : 2 * count], refs[-1]
    total = None
    for left, right in zip(lefts, rights):
        part = lax.dot_general(
            left[...], right[...], (((0,), (0,)), ((), ())), preferred_element_type=F32
        )
        total = part if total is None else total + part
    out[...] = total


def token_sum(lefts, rights):
    count = len(lefts)
    tokens, rows = lefts[0].shape
    cols = rights[0].shape[1]
    tile = 256 if rows % 256 == 0 else 128
    return pl.pallas_call(
        functools.partial(grad_kernel, count),
        grid=(rows // tile,),
        in_specs=[pl.BlockSpec((tokens, tile), lambda i: (0, i))] * count
        + [pl.BlockSpec((tokens, cols), lambda i: (0, 0))] * count,
        out_specs=pl.BlockSpec((tile, cols), lambda i: (i, 0)),
        out_shape=jax.ShapeDtypeStruct((rows, cols), F32),
        cost_estimate=pl.CostEstimate(
            flops=2 * count * tokens * rows * cols,
            bytes_accessed=2 * count * tokens * (rows + cols) + 4 * rows * cols,
            transcendentals=0,
        ),
        compiler_params=pltpu.CompilerParams(vmem_limit_bytes=32 << 20),
    )(*lefts, *rights)


def body(dp, tp, tokens, w_gate, w_up, w_down, cotangent):
    me = lax.axis_index("dp")
    part = tokens.shape[1] // dp

    def features(x, k):
        return lax.dynamic_slice_in_dim(x, (me ^ k) * part, part, axis=1)

    gathered = jnp.concatenate(gather_tp(tokens, tp), axis=0)
    gate = jnp.dot(gathered, w_gate, preferred_element_type=F32)
    up = jnp.dot(gathered, w_up, preferred_element_type=F32)

    grads = gather_tp(cotangent, tp)
    grad_full = jnp.concatenate(grads, axis=0)

    sig = jax.nn.sigmoid(gate)
    act = gate * sig
    hidden = (act * up).astype(BF16)
    back = right_trans(grad_full, w_down)
    dgate = (back * up * sig * (1.0 + gate * (1.0 - sig))).astype(BF16)
    dup = (back * act).astype(BF16)

    mixed = scatter_tp(jnp.dot(hidden, w_down, preferred_element_type=F32).astype(BF16), tp)
    input_grad = scatter_tp(
        (right_trans(dgate, w_gate) + right_trans(dup, w_up)).astype(BF16), tp
    )

    token_parts = [features(gathered, 0)] + [
        send_xor(features(gathered, k), k, dp) for k in range(1, dp)
    ]

    far = [send_xor(features(cotangent, k), k, dp) for k in range(2, dp)]
    rows = cotangent.shape[0]
    far = gather_tp(jnp.concatenate(far, axis=0), tp)
    grad_parts = [features(grad_full, 0), send_xor(features(grad_full, 1), 1, dp)] + [
        jnp.concatenate([f[i * rows : (i + 1) * rows] for f in far], axis=0) for i in range(dp - 2)
    ]

    all_hidden = gather_dp(hidden, dp)
    all_dgate = gather_dp(dgate, dp)
    all_dup = gather_dp(dup, dp)
    down_grad = token_sum(all_hidden, grad_parts)
    gate_grad = token_sum(token_parts, all_dgate)
    up_grad = token_sum(token_parts, all_dup)
    return (mixed, input_grad, gate_grad, up_grad, down_grad)


def solution(mesh):
    in_specs = (
        P(("dp", "tp"), None),
        P(None, "tp"),
        P(None, "tp"),
        P("tp", None),
        P(("dp", "tp"), None),
    )
    out_specs = (
        P(("dp", "tp"), None),
        P(("dp", "tp"), None),
        P("dp", "tp"),
        P("dp", "tp"),
        P("tp", "dp"),
    )
    run = functools.partial(body, mesh.shape["dp"], mesh.shape["tp"])
    return jax.shard_map(run, mesh=mesh, in_specs=in_specs, out_specs=out_specs, check_vma=False)
```
